32 devices in a mesh: rep: 4 (over x, y), dp: 8 (over z, core).
Axes of the slice: x: 2, y: 2, z: 4, core: 2. Of those that a mesh axis runs over, the one named last changes fastest.
Arguments:
- x: bfloat16 [32, 4096, 640], P(('rep', 'dp')), parts along dimension 0
- dy: bfloat16 [32, 4096, 640], P(('rep', 'dp')), parts along dimension 0
- w_gate: bfloat16 [2, 640, 2560], P(None, 'dp')
- w_up: bfloat16 [2, 640, 2560], P(None, 'dp')
- w_down: bfloat16 [2, 2560, 640], P(None, 'dp')
Outputs:
- output 1: bfloat16 [32, 4096, 640], P(('rep', 'dp')), parts along dimension 0
- output 2: bfloat16 [8, 640, 2560], P('rep', 'dp'), parts along dimension 0
- output 3: bfloat16 [8, 640, 2560], P('rep', 'dp'), parts along dimension 0
- output 4: bfloat16 [8, 2560, 640], P('rep', 'dp'), parts along dimension 0
There are 4 independent parts. The reference program is written for one: setup_inputs(seed, part) draws one part's arguments, and reference() takes and returns one part's arrays. A program takes and returns all parts, laid end to end along the dimension named above; an argument that names none is the same for every part.
All inputs are finite; a program needn't handle non-finite values.
Results may differ from the reference program's by a relative error of at most 0.018.
Values are sent between devices in bfloat16 or wider.
A program may use at most 2 GiB of HBM per device.

```python
import jax
import jax.numpy as jnp
from jax import lax

SEQUENCES = 8
TOKENS = 4096
D = 640
FF = 2560
LAYERS = 2
NAMES = ("w_gate", "w_up", "w_down")
SHAPES = {"w_gate": (LAYERS, D, FF), "w_up": (LAYERS, D, FF), "w_down": (LAYERS, FF, D)}


def bump(key, n, height):
    away = (jnp.arange(n, dtype=jnp.int32) - jax.random.randint(key, (), 0, n, jnp.int32)) % n
    return jnp.where(away < n // 8, height, 1.0)


def together(key, own, strength):
    shared = jax.random.normal(key, own.shape[1:], jnp.float32)
    return (own + strength * shared) * lax.rsqrt(1 + strength * strength)


def setup_inputs(seed: int = 0, part: int = 0) -> dict:
    kx, kdy, ka, kb, kz, kf, kh, kl, *kw = jax.random.split(jax.random.key(seed), 8 + len(NAMES))
    kx, kdy, ka, kb = (jax.random.fold_in(k, part) for k in (kx, kdy, ka, kb))
    shape = (SEQUENCES, TOKENS, D)
    much_x, much_dy = jax.random.uniform(kz, (2,), jnp.float32, 0.0, 1.0)
    layers = 2.0 ** jax.random.uniform(kl, (LAYERS, 1, 1), jnp.float32, -1.0, 1.0)
    x = together(ka, jax.random.normal(kx, shape, jnp.float32), much_x) * bump(kf, D, 4.0)
    dy = together(kb, jax.random.normal(kdy, shape, jnp.float32), much_dy)
    drawn = {"x": x.astype(jnp.bfloat16), "dy": (dy * (SEQUENCES * TOKENS) ** -0.5).astype(jnp.bfloat16)}
    for key, name in zip(kw, NAMES, strict=True):
        w = jax.random.normal(key, SHAPES[name], jnp.float32) * SHAPES[name][1] ** -0.5
        drawn[name] = (w * {"w_gate": 1.0, "w_up": bump(kh, FF, 4.0), "w_down": layers}[name]).astype(jnp.bfloat16)
    return drawn


def matmul(a, w):
    return jnp.dot(a, w, preferred_element_type=jnp.float32).astype(jnp.bfloat16)


def normed(h):
    wide = h.astype(jnp.float32)
    scale = lax.rsqrt(jnp.mean(wide**2, -1, keepdims=True) + 1e-6)
    return (wide * scale).astype(jnp.bfloat16)


def layer(h, w):
    a = normed(h)
    gate = jnp.dot(a, w["w_gate"], preferred_element_type=jnp.float32)
    up = jnp.dot(a, w["w_up"], preferred_element_type=jnp.float32)
    return h + matmul((jax.nn.silu(gate) * up).astype(jnp.bfloat16), w["w_down"])


def stack(weights, h):
    return lax.scan(lambda h, w: (layer(h, w), None), h, weights)[0]


def reference(x, dy, w_gate, w_up, w_down):
    weights = dict(zip(NAMES, (w_gate, w_up, w_down), strict=True))

    def take(so_far, sequence):
        h, by_y = sequence
        _, back = jax.vjp(stack, weights, h)
        by_weights, by_h = back(by_y)
        return jax.tree.map(lambda total, term: total + term.astype(jnp.float32), so_far, by_weights), by_h

    none_yet = {name: jnp.zeros(w.shape, jnp.float32) for name, w in weights.items()}
    by_weights, by_x = lax.scan(take, none_yet, (x, dy))
    return (by_x, *(by_weights[name].astype(jnp.bfloat16) for name in NAMES))
```

```python
import functools

import jax
import jax.numpy as jnp
from jax import lax
from jax.experimental import pallas as pl
from jax.experimental.pallas import tpu as pltpu
from jax.sharding import Mesh, PartitionSpec as P

GROUPS = ((0, 1), (2, 3, 4))
EXCHANGES = (0, 2, 4, 6)
NB = 5
TF = 512
TB = 512
SUB = 256
VMEM = 67_000_000
F32 = jnp.float32
BF16 = jnp.bfloat16
Z, C = 4, 2


def mm(a, b):
    return jnp.dot(a, b, preferred_element_type=F32)


def mm_nt(a, b):
    return lax.dot_general(a, b, (((1,), (1,)), ((), ())), preferred_element_type=F32)


def mm_tn(a, b):
    return lax.dot_general(a, b, (((0,), (0,)), ((), ())), preferred_element_type=F32)


def scale_of(wide):
    return lax.rsqrt(jnp.mean(wide * wide, -1, keepdims=True) + 1e-6)


def unpack(core_ref, mine_ref, other_ref, wg, wu, wd):
    dr = wg.shape[0] // (Z * C)
    fr = wd.shape[0] // (Z * C)
    for w_ref, c in ((mine_ref, core_ref[0]), (other_ref, 1 - core_ref[0])):
        for z in range(Z):
            rows = pl.ds(pl.multiple_of(z * C * dr + c * dr, 16), dr)
            for k in range(wg.shape[1] // 128):
                wg[rows, 128 * k : 128 * k + 128] = w_ref[z, 0, dr * k : dr * k + dr, :]
                wu[rows, 128 * k : 128 * k + 128] = w_ref[z, 1, dr * k : dr * k + dr, :]
            rows = pl.ds(pl.multiple_of(c * Z * fr + z * fr, 16), fr)
            for k in range(wd.shape[1] // 128):
                wd[rows, 128 * k : 128 * k + 128] = w_ref[z, 2, fr * k : fr * k + fr, :]


def forward_kernel(first, last, *refs):
    refs = list(refs)
    h_ref = refs.pop(0) if first or last else None
    a_ref = None if first else refs.pop(0)
    w_refs = [refs.pop(0) for _ in range(3)]
    acc_ref = None if first else refs.pop(0)
    gate_ref, up_ref = refs.pop(0), refs.pop(0)
    if first:
        a_out, acc_out = refs.pop(0), refs.pop(0)
    elif last:
        h_out, a_out = refs.pop(0), refs.pop(0)
    else:
        acc_out = refs.pop(0)
    wg, wu, wd = refs

    @pl.when(pl.program_id(0) == 0)
    def _():
        unpack(*w_refs, wg, wu, wd)

    for s in range(TF // SUB):
        rows = slice(s * SUB, s * SUB + SUB)
        if first:
            wide = h_ref[rows].astype(F32)
            a = (wide * scale_of(wide)).astype(BF16)
            a_out[rows] = a
        else:
            a = a_ref[rows]
        gate = mm(a, wg[...])
        up = mm(a, wu[...])
        gate_ref[rows] = gate
        up_ref[rows] = up
        sig = 0.5 * jnp.tanh(0.5 * gate) + 0.5
        p = (gate * sig * up).astype(BF16)
        o = mm(p, wd[...])
        if not first:
            o = o + acc_ref[rows]
        if last:
            h = h_ref[rows] + o.astype(BF16)
            h_out[rows] = h
            wide = h.astype(F32)
            a_out[rows] = (wide * scale_of(wide)).astype(BF16)
        else:
            acc_out[rows] = o


def backward_kernel(first, last, saved, *refs):
    refs = list(refs)
    a_ref, dy_ref = refs.pop(0), refs.pop(0)
    w_refs = [refs.pop(0) for _ in range(3)]
    if saved:
        gate_ref, up_ref = refs.pop(0), refs.pop(0)
    acc_ref = None if first else refs.pop(0)
    h_ref = refs.pop(0) if last else None
    dw_out, out = refs.pop(0), refs.pop(0)
    wg, wu, wd, dwg, dwu, dwd, p_s, dg_s, du_s = refs
    step = pl.program_id(0)

    @pl.when(step == 0)
    def _():
        unpack(*w_refs, wg, wu, wd)
        dwg[...] = jnp.zeros_like(dwg)
        dwu[...] = jnp.zeros_like(dwu)
        dwd[...] = jnp.zeros_like(dwd)

    for s in range(TB // SUB):
        rows = slice(s * SUB, s * SUB + SUB)
        dp = mm_nt(dy_ref[rows], wd[...]).astype(BF16).astype(F32)
        if saved:
            gate, up = gate_ref[rows], up_ref[rows]
        else:
            gate, up = mm(a_ref[rows], wg[...]), mm(a_ref[rows], wu[...])
        sig = 0.5 * jnp.tanh(0.5 * gate) + 0.5
        silu = gate * sig
        p_s[rows] = (silu * up).astype(BF16)
        du_s[rows] = (dp * silu).astype(BF16)
        dg_s[rows] = (dp * up * (sig + silu * (1.0 - sig))).astype(BF16)
        da = mm_nt(dg_s[rows], wg[...]) + mm_nt(du_s[rows], wu[...])
        if not first:
            da = da + acc_ref[rows]
        if last:
            da = da.astype(BF16).astype(F32)
            wide = h_ref[rows].astype(F32)
            r = scale_of(wide)
            inner = jnp.mean(da * wide, -1, keepdims=True)
            dh = da * r - wide * (r * r * r * inner)
            out[rows] = dy_ref[rows] + dh.astype(BF16)
        else:
            out[rows] = da
    dwg[...] += mm_tn(a_ref[...], dg_s[...])
    dwu[...] += mm_tn(a_ref[...], du_s[...])
    dwd[...] += mm_tn(dy_ref[...], p_s[...])

    @pl.when(step == pl.num_programs(0) - 1)
    def _():
        dr = dwg.shape[0] // (Z * C)
        fr = dwd.shape[1] // (Z * C)
        for k in range(dwg.shape[1] // 128):
            for c in range(C):
                for z in range(Z):
                    r = (z * C + c) * dr
                    dw_out[c, z, 0, dr * k : dr * k + dr, :] = dwg[r : r + dr, 128 * k : 128 * k + 128].astype(BF16)
                    dw_out[c, z, 1, dr * k : dr * k + dr, :] = dwu[r : r + dr, 128 * k : 128 * k + 128].astype(BF16)
        for k in range(dwd.shape[0] // 128):
            block = jnp.transpose(dwd[128 * k : 128 * k + 128, :]).astype(BF16)
            for c in range(C):
                for z in range(Z):
                    r = (c * Z + z) * fr
                    dw_out[c, z, 2, fr * k : fr * k + fr, :] = block[r : r + fr, :]


def rows_spec(t, width):
    return pl.BlockSpec((t, width), lambda i: (i, 0))


def whole_spec(shape):
    return pl.BlockSpec(shape, lambda i: (0,) * len(shape))


def params():
    return pltpu.CompilerParams(dimension_semantics=("arbitrary",), vmem_limit_bytes=VMEM)


def weights_scratch(d, fb):
    return [pltpu.VMEM((d, fb), BF16), pltpu.VMEM((d, fb), BF16), pltpu.VMEM((fb, d), BF16)]


def weights_args(w):
    core, mine, other, n = w
    spec = pl.BlockSpec((Z, None, *mine.shape[2:]), lambda i: (0, n, 0, 0, 0))
    return [core, mine, other], [pl.BlockSpec(memory_space=pltpu.SMEM), spec, spec]


def forward(first, last, h, a, w, acc, fb):
    n, d = h.shape
    full = jax.ShapeDtypeStruct
    args, specs = [], []
    if first or last:
        args.append(h)
        specs.append(rows_spec(TF, d))
    if not first:
        args.append(a)
        specs.append(rows_spec(TF, d))
    w_args, w_specs = weights_args(w)
    args += w_args
    specs += w_specs
    alias = {}
    outs = [(full((n, fb), F32), rows_spec(TF, fb))] * 2
    if first:
        outs += [(full((n, d), BF16), rows_spec(TF, d)), (full((n, d), F32), rows_spec(TF, d))]
    elif last:
        outs += [(full((n, d), BF16), rows_spec(TF, d))] * 2
    else:
        outs += [(full((n, d), F32), rows_spec(TF, d))]
    if not first:
        if not last:
            alias = {len(args): 2}
        args.append(acc)
        specs.append(rows_spec(TF, d))
    return pl.pallas_call(
        functools.partial(forward_kernel, first, last),
        grid=(n // TF,),
        out_shape=[o for o, _ in outs],
        in_specs=specs,
        out_specs=[s for _, s in outs],
        scratch_shapes=weights_scratch(d, fb),
        input_output_aliases=alias,
        compiler_params=params(),
        cost_estimate=pl.CostEstimate(flops=6 * n * d * fb, bytes_accessed=n * (16 * d + 8 * fb), transcendentals=n * fb),
        name="mlp_fwd",
    )(*args)


def backward(first, last, saved, a, dy, w, gates, acc, h, fb):
    n, d = a.shape
    w_args, w_specs = weights_args(w)
    grad = (C, Z, *w_args[1].shape[2:])
    full = jax.ShapeDtypeStruct
    args, specs = [a, dy, *w_args], [rows_spec(TB, d), rows_spec(TB, d), *w_specs]
    if saved:
        args += list(gates)
        specs += [rows_spec(TB, fb)] * 2
    alias = {}
    if not first:
        if not last:
            alias = {len(args): 1}
        args.append(acc)
        specs.append(rows_spec(TB, d))
    if last:
        args.append(h)
        specs.append(rows_spec(TB, d))
    return pl.pallas_call(
        functools.partial(backward_kernel, first, last, saved),
        grid=(n // TB,),
        out_shape=[full(grad, BF16), full((n, d), BF16 if last else F32)],
        in_specs=specs,
        out_specs=[whole_spec(grad), rows_spec(TB, d)],
        scratch_shapes=weights_scratch(d, fb) + [pltpu.VMEM((d, fb), F32)] * 3 + [pltpu.VMEM((TB, fb), BF16)] * 3,
        input_output_aliases=alias,
        compiler_params=params(),
        cost_estimate=pl.CostEstimate(
            flops=(12 if saved else 16) * n * d * fb, bytes_accessed=n * (12 * d + (8 * fb if saved else 0)), transcendentals=n * fb
        ),
        name="mlp_bwd",
    )(*args)


def pack_kernel(layers, groups, wg_ref, wu_ref, wd_ref, *outs):
    dr = wg_ref.shape[1]
    fr = wd_ref.shape[1] // NB
    span = NB * fr
    for l in range(layers):
        for g, group in enumerate(groups):
            out = outs[l * len(groups) + g]
            for n, j in enumerate(group):
                for m, ref in enumerate((wg_ref, wu_ref)):
                    for k in range(Z * C * fr // 128):
                        c, z = divmod(2 * k, Z)
                        pieces = []
                        for zz in (z, z + 1):
                            start = (zz * C + c) * span + fr * j
                            pieces.append(ref[l, :, start : start + fr])
                        out[n, m, dr * k : dr * k + dr, :] = jnp.concatenate(pieces, 1)
                for k in range(wd_ref.shape[2] // 128):
                    out[n, 2, fr * k : fr * k + fr, :] = wd_ref[l, fr * j : fr * j + fr, 128 * k : 128 * k + 128]


def pack(wg, wu, wd, groups):
    layers = wg.shape[0]
    rows = wg.shape[1] * wg.shape[2] // NB // 128
    shapes = [jax.ShapeDtypeStruct((len(group), 3, rows, 128), BF16) for _ in range(layers) for group in groups]
    outs = pl.pallas_call(
        functools.partial(pack_kernel, layers, groups),
        out_shape=shapes,
        compiler_params=pltpu.CompilerParams(vmem_limit_bytes=VMEM),
        name="pack",
    )(wg, wu, wd)
    return [outs[l * len(groups) : (l + 1) * len(groups)] for l in range(layers)]


def unpack_grads_kernel(layers, *refs):
    gs, (og, ou, od) = refs[: layers * NB], refs[layers * NB :]
    dr = og.shape[1]
    fr = od.shape[1] // NB
    for l in range(layers):
        for j in range(NB):
            g = gs[l * NB + j]
            for m, out in enumerate((og, ou)):
                for k in range(Z * C * fr // 128):
                    c, z = divmod(2 * k, Z)
                    rows = g[m, dr * k : dr * k + dr, :]
                    for half, zz in enumerate((z, z + 1)):
                        start = (zz * C + c) * NB * fr + fr * j
                        out[l, :, start : start + fr] = rows[:, half * fr : half * fr + fr]
            for k in range(od.shape[2] // 128):
                od[l, fr * j : fr * j + fr, 128 * k : 128 * k + 128] = g[2, fr * k : fr * k + fr, :]


def unpack_grads(grads, dr, ff, d):
    layers = len(grads)
    full = jax.ShapeDtypeStruct
    return pl.pallas_call(
        functools.partial(unpack_grads_kernel, layers),
        out_shape=[full((layers, dr, ff), BF16)] * 2 + [full((layers, ff // Z // C, d), BF16)],
        compiler_params=pltpu.CompilerParams(vmem_limit_bytes=VMEM),
        name="unpack",
    )(*[g for layer in grads for g in layer])


def solution(mesh):
    split = Mesh(mesh.devices.reshape(mesh.devices.shape[0], Z, C), ("rep", "z", "core"))

    def body(x, dy, wg, wu, wd):
        layers, dr, ff = wg.shape
        d = x.shape[-1]
        fb = ff // NB
        x, dy = x[0], dy[0]
        core = lax.axis_index("core").astype(jnp.int32).reshape(1)
        packed = [w for layer in pack(wg, wu, wd, GROUPS) for w in layer]
        mine = [lax.all_gather(w, "z") for w in packed]
        gathered = {}
        runs = 0

        def before_kernel(*values):
            nonlocal runs
            for g, run in enumerate(EXCHANGES):
                if run == runs:
                    if run:
                        mine[g], *values = lax.optimization_barrier((mine[g], *values))
                    other = lax.ppermute(mine[g], "core", [(0, 1), (1, 0)])
                    for n, j in enumerate(GROUPS[g % len(GROUPS)]):
                        gathered[g // len(GROUPS), j] = (core, mine[g], other, n)
            runs += 1
            return values

        hs, as_, gates = [x], [], []
        h = x
        a = acc = None
        for l in range(layers - 1):
            gates.append([])
            for j in range(NB):
                first, last = j == 0 and l == 0, j == NB - 1
                (acc,) = before_kernel(acc)
                gate, up, *rest = forward(first, last, h, a, gathered[l, j], acc, fb)
                gates[l].append((gate, up))
                if first:
                    a, acc = rest
                    as_.append(a)
                elif last:
                    h, a = rest
                    hs.append(h)
                    as_.append(a)
                else:
                    (acc,) = rest

        over_core, over_z = [], []
        by_h = dy
        for l in reversed(range(layers)):
            acc = None
            for j in range(NB):
                saved = l < layers - 1
                k = len(over_core)
                by_h, acc = before_kernel(by_h, acc)
                while len(over_z) <= k - 2:
                    n = len(over_z)
                    done = over_z[n - 1] if n else None
                    by_h, acc, over_core[n], done = lax.optimization_barrier((by_h, acc, over_core[n], done))
                    if n:
                        over_z[n - 1] = done
                    over_z.append(lax.psum_scatter(over_core[n], "z", scatter_dimension=0, tiled=False))
                dw, acc = backward(
                    j == 0, j == NB - 1, saved, as_[l], by_h, gathered[l, j], gates[l][j] if saved else None, acc, hs[l], fb
                )
                over_core.append(lax.psum_scatter(dw, "core", scatter_dimension=0, tiled=False))
            by_h = acc
        for part in over_core[len(over_z) :]:
            over_z.append(lax.psum_scatter(part, "z", scatter_dimension=0, tiled=False))
        grads = [over_z[NB * (layers - 1 - l) :][:NB] for l in range(layers)]
        return (by_h[None], *unpack_grads(grads, dr, ff, d))

    rows, weights, outs = P(("rep", "z", "core")), P(None, ("z", "core")), P("rep", ("z", "core"))
    return jax.shard_map(
        body, mesh=split, in_specs=(rows, rows, weights, weights, weights), out_specs=(rows, outs, outs, outs), check_vma=False
    )
```
